32 devices in a mesh: ctx: 16 (over z, y, x), head: 2 (over core).
Axes of the slice: x: 2, y: 2, z: 4, core: 2. Of those that a mesh axis runs over, the one named last changes fastest.
Arguments:
- queries: bfloat16 [8192, 2048], P('ctx', 'head'), may hold values from -24 to 24
- keys: bfloat16 [8192, 2048], P('ctx', 'head'), may hold values from -24 to 24
- values: bfloat16 [8192, 2048], P('ctx', 'head'), may hold values from -6 to 6
- prefix_keys: bfloat16 [8192, 2048], P('ctx', 'head'), may hold values from -6 to 6
- prefix_values: bfloat16 [8192, 2048], P('ctx', 'head'), may hold values from -6 to 6
- selected: int32 [2, 64, 8, 3], P('head', 'ctx'), may hold values from 0 to 15, all different within a row; in each aligned block of 32 rows (0 to 31, 32 to 63, ..., all dimensions but the last counted through in order) at most 6 rows name the same one
- out_weight: bfloat16 [2, 1024, 4096], P('head', 'ctx'), may hold values from -0.125 to 0.125
Outputs:
- mixed: bfloat16 [8192, 4096], P('ctx', 'head')
The draws below stay inside these ranges and needn't reach their ends.
Inputs may be any that keep to these rules, and one draw needn't show every extreme that they name: `selected`: for every head group, tile and head, 3 different prefix blocks. Among the 32 rows of one device (one head group, that device's tiles), no block is named more than 6 times.
All inputs are finite; a program needn't handle non-finite values.
Results may differ from the reference program's by a relative error of at most 0.0056.
Values may be sent and summed in bfloat16 or wider, within the bound.
No kernel may reach another device: no remote copies, remote signals or barrier semaphores. Data moves between devices by JAX's collectives and lax.ppermute only.
A program may use at most 128 MiB of HBM per device.

```python
import math
import jax
import jax.numpy as jnp
import numpy as np
from jax import lax

D = 4096
HEADS = 16
D_HEAD = 128
TILE = 128
BLOCK = 512
TOPK = 3
HEADS_DEV = 8
GROUPS = 2
TILES_DEV = 4
NEW_TOKENS = 8192
PREFIX_TOKENS = 8192
TILES = 64
PREFIX_BLOCKS = 16
CAP = 6


def drawn_base(key, salt):
    drawn = jax.random.normal(jax.random.fold_in(key, salt), (NEW_TOKENS, HEADS * D_HEAD), jnp.float32)
    return jnp.clip(drawn, -6.0, 6.0)


def draw_queries(key, part):
    drawn = drawn_base(key, 1)
    return drawn.astype(jnp.bfloat16)


def draw_keys(key, part):
    drawn = drawn_base(key, 2)
    return drawn.astype(jnp.bfloat16)


def block_levels(stream_key, shape, cuts, smallest, high):
    loudness = 1.0
    for dim, blocks in cuts:
        heights = jax.random.uniform(jax.random.fold_in(jax.random.fold_in(stream_key, 6), dim), (blocks,), jnp.float32, smallest / len(cuts), high / len(cuts))
        loudness = loudness * jnp.repeat(jnp.exp(heights), shape[dim] // blocks).reshape((-1,) + (1,) * (len(shape) - 1 - dim))
    return loudness


def shared_out(key, own, number, rows, number_of, top, most, lean):
    sequence = jax.random.permutation(key, number_of)
    packed, common = load_shares(number_of, rows * top, most, lean, True), load_shares(number_of, rows * top, most, lean, False)
    places = jnp.arange(number_of)

    def named(sizes, turn):
        used = int((sizes > 0).sum())
        fixed = max(1, used // 4)
        moved = fixed + (places - fixed + turn * (used - fixed)) % max(1, number_of - fixed)
        return jnp.zeros((number_of,), jnp.int32).at[sequence[jnp.where(places < fixed, places, moved)]].set(jnp.asarray(sizes, jnp.int32))

    sizes = jnp.where(number % 4 == 0, named(packed, number // 4), named(common, number - number // 4 - 1))
    mixed = jax.random.permutation(jax.random.fold_in(own, 3), number_of)
    giver, sink = mixed[0:number_of // 2 * 2:2], mixed[1:number_of // 2 * 2:2]
    room = jnp.minimum(sizes[giver] - 1, most - sizes[sink]) // 2
    room = jnp.where((giver == sequence[0]) | (sink == sequence[0]) | (sizes[sink] == 0), 0, jnp.maximum(room, 0))
    moved = jax.random.randint(jax.random.fold_in(own, 4), (number_of // 2,), 0, 1 << 20) % (room + 1)
    sizes = sizes.at[giver].add(-moved).at[sink].add(moved)
    members = jnp.searchsorted(jnp.cumsum(sizes), jnp.arange(rows * top), side="right").astype(jnp.int32)
    table = members.reshape(top, rows).T
    table = table[jax.random.permutation(jax.random.fold_in(own, 1), rows)]
    turn = jax.random.randint(jax.random.fold_in(own, 2), (rows, 1), 0, top)
    return jnp.take_along_axis(table, (jnp.arange(top)[None, :] + turn) % top, axis=1)


def load_shares(amount, total, reach, lean, full):
    weights = [(1 << 20) // math.isqrt(grade ** lean) + 1 for grade in range(1, amount + 1)]
    largest = reach if full else min(reach, max(-(-total // amount), total * weights[0] // sum(weights)))
    least = 1 if total - largest >= amount - 1 else 0
    holding, surplus = [largest] + [least] * (amount - 1), total - largest - least * (amount - 1)
    while surplus > 0:
        free = [i for i in range(1, amount) if holding[i] < largest] or [i for i in range(1, amount) if holding[i] < reach]
        mass, budget = sum([weights[i] for i in free]), surplus
        for i in free:
            addition = min(reach - holding[i], max(1, budget * weights[i] // mass), surplus)
            holding[i] = holding[i] + addition
            surplus = surplus - addition
    return np.array(holding)


def bell_draw(own_key, extent, deviation, reach, pieces=(), kind=jnp.bfloat16):
    values = jax.random.normal(own_key, extent, jnp.float32) * deviation
    if len(pieces) > 0:
        values = block_levels(own_key, extent, pieces, -0.22, 0.18) * values
    return jnp.clip(values, min=-reach, max=reach).astype(kind)


def setup_inputs(seed: int = 0) -> dict:
    streams_of = jax.random.split(jax.random.key(seed), 8)
    queries = draw_queries(jax.random.fold_in(streams_of[7], 71), 0)
    keys = draw_keys(jax.random.fold_in(streams_of[7], 71), 0)
    values = bell_draw(streams_of[2], (NEW_TOKENS, HEADS * D_HEAD), 1.0, 6.0, ((0, 16), (1, 2)))
    prefix_keys = bell_draw(streams_of[3], (PREFIX_TOKENS, HEADS * D_HEAD), 1.0, 6.0, ((0, 16), (1, 2)))
    prefix_values = bell_draw(streams_of[4], (PREFIX_TOKENS, HEADS * D_HEAD), 1.0, 6.0, ((0, 16), (1, 2)))
    selected_keys = jax.random.split(jax.random.fold_in(streams_of[5], 1), GROUPS * TILES * HEADS_DEV // (TILES_DEV * HEADS_DEV))
    selected_turns = jax.random.permutation(jax.random.fold_in(streams_of[5], 3), GROUPS * TILES * HEADS_DEV // (TILES_DEV * HEADS_DEV))
    selected = jax.vmap(lambda own, number: shared_out(jax.random.fold_in(streams_of[5], 2), own, number, TILES_DEV * HEADS_DEV, PREFIX_BLOCKS, TOPK, CAP, 2))(selected_keys, selected_turns).reshape((GROUPS, TILES, HEADS_DEV, TOPK))
    out_weight = bell_draw(streams_of[6], (GROUPS, HEADS_DEV * D_HEAD, D), (HEADS * D_HEAD) ** -0.5, 0.125, ((0, 2), (1, 16)))
    return dict(queries=queries, keys=keys, values=values, prefix_keys=prefix_keys, prefix_values=prefix_values, selected=selected, out_weight=out_weight)


def rounded(weights):
    narrow = weights.astype(jnp.bfloat16)
    narrow = lax.optimization_barrier(narrow)
    return narrow.astype(jnp.float32)


def reference(queries, keys, values, prefix_keys, prefix_values, selected, out_weight):
    score_scale = D_HEAD ** -0.5
    query_heads = queries.reshape(NEW_TOKENS, HEADS, D_HEAD)
    key_heads = keys.reshape(NEW_TOKENS, HEADS, D_HEAD)
    value_heads = values.reshape(NEW_TOKENS, HEADS, D_HEAD)
    prefix_key_table = prefix_keys.reshape(PREFIX_BLOCKS, BLOCK, HEADS, D_HEAD).transpose(0, 2, 1, 3)
    prefix_value_table = prefix_values.reshape(PREFIX_BLOCKS, BLOCK, HEADS, D_HEAD).transpose(0, 2, 1, 3)
    picked = selected.transpose(1, 0, 2, 3).reshape(TILES, HEADS, TOPK)
    head_ids = jnp.arange(HEADS, dtype=jnp.int32)

    def one_tile(tile_index):
        row_start = (tile_index * TILE).astype(jnp.int32)
        block_start = ((row_start // BLOCK) * BLOCK).astype(jnp.int32)
        query_tile = lax.dynamic_slice_in_dim(query_heads, row_start, TILE, 0).astype(jnp.float32)
        own_keys = lax.dynamic_slice_in_dim(key_heads, block_start, BLOCK, 0).astype(jnp.float32)
        own_values = lax.dynamic_slice_in_dim(value_heads, block_start, BLOCK, 0).astype(jnp.float32)
        scores = jnp.einsum("qhd,khd->hqk", query_tile, own_keys) * score_scale
        query_pos = row_start + jnp.arange(TILE, dtype=jnp.int32)
        key_pos = block_start + jnp.arange(BLOCK, dtype=jnp.int32)
        visible = key_pos[None, :] <= query_pos[:, None]
        scores = jnp.where(visible[None, :, :], scores, -jnp.inf)
        own_max = jnp.max(scores, axis=2)
        own_weights = jnp.exp(scores - own_max[:, :, None])
        own_sum = jnp.sum(own_weights, axis=2)
        own_out = jnp.einsum("hqk,khd->hqd", rounded(own_weights), own_values)
        tile_picks = picked[tile_index]
        sel_keys = prefix_key_table[tile_picks, head_ids[:, None]].astype(jnp.float32)
        sel_values = prefix_value_table[tile_picks, head_ids[:, None]].astype(jnp.float32)
        sel_scores = jnp.einsum("qhd,hjkd->hjqk", query_tile, sel_keys) * score_scale
        sel_max = jnp.max(sel_scores, axis=3)
        sel_weights = jnp.exp(sel_scores - sel_max[:, :, :, None])
        sel_sum = jnp.sum(sel_weights, axis=3)
        sel_out = jnp.einsum("hjqk,hjkd->hjqd", rounded(sel_weights), sel_values)
        highest = jnp.maximum(own_max, jnp.max(sel_max, axis=1))
        own_factor = jnp.exp(own_max - highest)
        sel_factor = jnp.exp(sel_max - highest[:, None, :])
        numerator = own_factor[:, :, None] * own_out + jnp.sum(sel_factor[:, :, :, None] * sel_out, axis=1)
        denominator = own_factor * own_sum + jnp.sum(sel_factor * sel_sum, axis=1)
        result = numerator / denominator[:, :, None]
        return result.transpose(1, 0, 2).reshape(TILE, HEADS * D_HEAD).astype(jnp.bfloat16)

    attention = lax.map(one_tile, jnp.arange(TILES, dtype=jnp.int32)).reshape(NEW_TOKENS, HEADS * D_HEAD)
    full_weight = out_weight.reshape(HEADS * D_HEAD, D)
    return jnp.dot(attention, full_weight, preferred_element_type=jnp.float32).astype(jnp.bfloat16)
```

```python
import math

import jax
import jax.numpy as jnp
from jax import lax
from jax.experimental import pallas as pl
from jax.experimental.pallas import tpu as pltpu
from jax.sharding import PartitionSpec as P

D_HEAD = 128
TILE = 128
BLOCK = 512
TOPK = 3
SCALE = D_HEAD ** (-0.5)
LOG2E = 1.4426950408889634
BF16 = jnp.bfloat16
F32 = jnp.float32


def round_up(n, m):
    return (n + m - 1) // m * m


def smem():
    return pl.BlockSpec(memory_space=pltpu.SMEM)


def route_queries(picked, queries, peers, slots, blocks_here):
    tok_rows, width = queries.shape
    heads = width // D_HEAD
    requests = picked.shape[0]
    tail = round_up(slots, 16)
    rows = slots * TILE + tail
    steps = 4 if peers % 4 == 0 else 1
    per_step = peers // steps
    full = peers * slots == requests

    def body(picked_ref, q_ref, out_ref, owner_ref, rank_ref, source, pair, count):
        step = pl.program_id(0)

        @pl.when(step == 0)
        def _():
            for p in range(peers):
                count[p] = 0
            if not full:
                for i in range(peers * slots):
                    source[i] = -1
                    pair[i] = 0
            for r in range(requests):
                block = picked_ref[r]
                owner = block // blocks_here if blocks_here > 1 else block
                local = block % blocks_here if blocks_here > 1 else 0
                rank = count[owner]
                slot = owner * slots + rank
                source[slot] = r // TOPK
                pair[slot] = local * heads + (r // TOPK) % heads
                count[owner] = rank + 1
                owner_ref[r] = owner
                rank_ref[r] = rank

        sub = lax.broadcasted_iota(jnp.int32, (tail, TILE), 0)
        for i in range(per_step):
            ids = jnp.zeros((tail, TILE), F32)
            for s in range(slots):
                slot = (step * per_step + i) * slots + s
                row = source[slot]
                safe = row if full else jnp.maximum(row, 0)
                start = pl.multiple_of((safe // heads) * TILE, TILE)
                lane = pl.multiple_of((safe % heads) * D_HEAD, D_HEAD)
                q = q_ref[pl.ds(start, TILE), pl.ds(lane, D_HEAD)]
                if not full:
                    q = jnp.where(row >= 0, q, jnp.zeros_like(q))
                out_ref[i, s * TILE : (s + 1) * TILE, :] = q
                ids = jnp.where(sub == s, pair[slot].astype(F32), ids)
            out_ref[i, slots * TILE :, :] = ids.astype(BF16)

    return pl.pallas_call(
        body,
        grid=(steps,),
        in_specs=[smem(), pl.BlockSpec((tok_rows, width), lambda i: (0, 0))],
        out_specs=[pl.BlockSpec((per_step, rows, TILE), lambda i: (i, 0, 0)), smem(), smem()],
        out_shape=[
            jax.ShapeDtypeStruct((peers, rows, TILE), BF16),
            jax.ShapeDtypeStruct((requests,), jnp.int32),
            jax.ShapeDtypeStruct((requests,), jnp.int32),
        ],
        scratch_shapes=[
            pltpu.SMEM((peers * slots,), jnp.int32),
            pltpu.SMEM((peers * slots,), jnp.int32),
            pltpu.SMEM((peers,), jnp.int32),
        ],
        name="route",
    )(picked, queries)


def soft(scores):
    top = jnp.max(scores, axis=0, keepdims=True)
    weights = jnp.exp2((scores - top) * (SCALE * LOG2E))
    total = jnp.sum(weights, axis=0, keepdims=True)
    return weights.astype(BF16), total, top * SCALE + jnp.log(total)


def dot_nt(a, b):
    return lax.dot_general(a, b, (((1,), (1,)), ((), ())), preferred_element_type=F32)


def attend_slots(pairs, incoming, keys, values_t, slots, heads):
    peers, rows, _ = incoming.shape
    tail = round_up(3 * slots, 16)
    out_rows = slots * TILE + tail
    blocks = keys.shape[0] // BLOCK

    def body(pair_ref, q_ref, k_ref, v_ref, out_ref):
        p = pl.program_id(0)
        sub = lax.broadcasted_iota(jnp.int32, (tail, TILE), 0)
        logs = jnp.zeros((tail, TILE), F32)
        for s in range(slots):
            pair = pair_ref[p * slots + s]
            head = pair % heads if blocks > 1 else pair
            start = pl.multiple_of(pair // heads * BLOCK, BLOCK) if blocks > 1 else 0
            lane = pl.multiple_of(head * D_HEAD, D_HEAD)
            k = k_ref[pl.ds(start, BLOCK), pl.ds(lane, D_HEAD)]
            v = v_ref[pl.ds(lane, D_HEAD), pl.ds(start, BLOCK)]
            q = q_ref[0, s * TILE : (s + 1) * TILE, :]
            weights, total, lse = soft(dot_nt(k, q))
            out = jnp.dot(v, weights, preferred_element_type=F32) / total
            out_ref[0, s * TILE : (s + 1) * TILE, :] = out.astype(BF16)
            high = lse.astype(BF16).astype(F32)
            middle = (lse - high).astype(BF16).astype(F32)
            low = lse - high - middle
            logs = jnp.where(sub == 3 * s, high, logs)
            logs = jnp.where(sub == 3 * s + 1, middle, logs)
            logs = jnp.where(sub == 3 * s + 2, low, logs)
        out_ref[0, slots * TILE :, :] = logs.astype(BF16)

    return pl.pallas_call(
        body,
        grid=(peers,),
        in_specs=[
            smem(),
            pl.BlockSpec((1, rows, TILE), lambda i: (i, 0, 0)),
            pl.BlockSpec(keys.shape, lambda i: (0, 0)),
            pl.BlockSpec(values_t.shape, lambda i: (0, 0)),
        ],
        out_specs=pl.BlockSpec((1, out_rows, TILE), lambda i: (i, 0, 0)),
        out_shape=jax.ShapeDtypeStruct((peers, out_rows, TILE), BF16),
        name="attend",
    )(pairs, incoming, keys, values_t)


def own_attention(queries, keys, values_t):
    tok_rows, width = queries.shape
    heads = width // D_HEAD
    blocks = tok_rows // BLOCK

    def body(q_ref, k_ref, v_ref, out_ref, lse_ref):
        for t in range(BLOCK // TILE):
            seen = (t + 1) * TILE
            scores = dot_nt(k_ref[:seen, :], q_ref[t * TILE : seen, :])
            key = lax.broadcasted_iota(jnp.int32, scores.shape, 0)
            query = lax.broadcasted_iota(jnp.int32, scores.shape, 1) + t * TILE
            weights, total, lse = soft(jnp.where(key <= query, scores, -jnp.inf))
            out = jnp.dot(v_ref[:, :seen], weights, preferred_element_type=F32) / total
            out_ref[:, t * TILE : seen] = out
            lse_ref[0, :, t * TILE : seen] = lse

    block = pl.BlockSpec((BLOCK, D_HEAD), lambda b, h: (b, h))
    block_t = pl.BlockSpec((D_HEAD, BLOCK), lambda b, h: (h, b))
    return pl.pallas_call(
        body,
        grid=(blocks, heads),
        in_specs=[block, block, block_t],
        out_specs=[block_t, pl.BlockSpec((1, 1, BLOCK), lambda b, h: (h, 0, b))],
        out_shape=[
            jax.ShapeDtypeStruct((width, tok_rows), F32),
            jax.ShapeDtypeStruct((heads, 1, tok_rows), F32),
        ],
        name="own",
    )(queries, keys, values_t)


def combine(owner, rank, place, back, own_out, own_lse, slots):
    peers, rows, _ = back.shape
    width, tok_rows = own_out.shape
    heads = width // D_HEAD
    tiles = tok_rows // TILE
    chunk = width // peers
    tail = rows - slots * TILE

    def body(owner_ref, rank_ref, place_ref, back_ref, out_ref, lse_ref, att_ref, turned):
        t = pl.program_id(0)
        sub = lax.broadcasted_iota(jnp.int32, (tail, TILE), 0)
        for h in range(heads):
            logs, parts = [lse_ref[h]], [out_ref[h * D_HEAD : (h + 1) * D_HEAD, :]]
            for j in range(TOPK):
                r = (t * heads + h) * TOPK + j
                p, s = owner_ref[r], rank_ref[r]
                start = pl.multiple_of(s * TILE, TILE)
                parts.append(back_ref[p, pl.ds(start, TILE), :].astype(F32))
                terms = back_ref[p, slots * TILE :, :].astype(F32)
                mine = jnp.logical_and(sub >= 3 * s, sub < 3 * s + 3)
                logs.append(jnp.sum(jnp.where(mine, terms, 0.0), axis=0, keepdims=True))
            top = logs[0]
            for log in logs[1:]:
                top = jnp.maximum(top, log)
            factors = [jnp.exp(log - top) for log in logs]
            inverse = 1.0 / (factors[0] + factors[1] + factors[2] + factors[3])
            mixed = parts[0] * (factors[0] * inverse)
            for factor, part in zip(factors[1:], parts[1:]):
                mixed = mixed + part * (factor * inverse)
            for i in range(D_HEAD // chunk):
                at = pl.multiple_of(place_ref[h * (D_HEAD // chunk) + i] * chunk, chunk)
                turned[pl.ds(at, chunk), :] = mixed[i * chunk : (i + 1) * chunk, :]
        for h in range(heads):
            lanes = slice(h * D_HEAD, (h + 1) * D_HEAD)
            att_ref[:, lanes] = turned[lanes, :].T.astype(BF16)

    return pl.pallas_call(
        body,
        grid=(tiles,),
        in_specs=[
            smem(),
            smem(),
            smem(),
            pl.BlockSpec(back.shape, lambda i: (0, 0, 0)),
            pl.BlockSpec((width, TILE), lambda i: (0, i)),
            pl.BlockSpec((heads, 1, TILE), lambda i: (0, 0, i)),
        ],
        out_specs=pl.BlockSpec((TILE, width), lambda i: (i, 0)),
        out_shape=jax.ShapeDtypeStruct((tok_rows, width), BF16),
        scratch_shapes=[pltpu.VMEM((width, TILE), F32)],
        name="combine",
    )(owner, rank, place, back, own_out, own_lse)


def project(att_own, att_other, w_own, w_other):
    rows, depth = att_own.shape
    width = w_own.shape[1]
    part = min(width, 512)

    def body(a_ref, b_ref, wa_ref, wb_ref, out_ref):
        total = jnp.dot(a_ref[...], wa_ref[...], preferred_element_type=F32)
        total += jnp.dot(b_ref[...], wb_ref[...], preferred_element_type=F32)
        out_ref[...] = total.astype(BF16)

    held = pl.BlockSpec((rows, depth), lambda i: (0, 0))
    weight = pl.BlockSpec((depth, part), lambda i: (0, i))
    return pl.pallas_call(
        body,
        grid=(width // part,),
        in_specs=[held, held, weight, weight],
        out_specs=pl.BlockSpec((rows, part), lambda i: (0, i)),
        out_shape=jax.ShapeDtypeStruct((rows, width), BF16),
        name="project",
    )(att_own, att_other, w_own, w_other)


def bit_orders(peers):
    bits = int(math.log2(peers))
    high = list(range(bits - 1, 1, -1))
    return [high + [1, 0], high + [0, 1]]


def doubling_pairs(peers, orders, step, other):
    pairs = []
    for c in range(peers):
        for h in range(2):
            group = 1 - h if other else h
            pairs.append((2 * c + h, 2 * (c ^ (1 << orders[group][step])) + h))
    return pairs


def shards(queries, keys, values, prefix_keys, prefix_values, selected, out_weight):
    tok_rows, width = queries.shape
    heads = width // D_HEAD
    tiles = tok_rows // TILE
    blocks_here = prefix_keys.shape[0] // BLOCK
    peers = lax.axis_size("ctx")
    me, core = lax.axis_index("ctx"), lax.axis_index("head")
    requests = tiles * heads * TOPK
    capacity = -(-requests // (peers * blocks_here))
    slots = capacity * blocks_here
    swap = [(0, 1), (1, 0)]

    outgoing, owner, rank = route_queries(
        selected.reshape(requests), queries, peers, slots, blocks_here
    )
    incoming = lax.all_to_all(outgoing, "ctx", split_axis=0, concat_axis=0, tiled=True)

    half = out_weight.shape[2] // 2
    weight = out_weight[0]
    w_own = lax.dynamic_slice_in_dim(weight, core * half, half, 1)
    w_other = lax.ppermute(
        lax.dynamic_slice_in_dim(weight, (1 - core) * half, half, 1), "head", swap
    )
    orders = bit_orders(peers)
    for step in range(len(orders[0])):
        got = lax.ppermute(w_own, ("ctx", "head"), doubling_pairs(peers, orders, step, False))
        w_own = jnp.concatenate([w_own, got], axis=0)
        got = lax.ppermute(w_other, ("ctx", "head"), doubling_pairs(peers, orders, step, True))
        w_other = jnp.concatenate([w_other, got], axis=0)

    apart = jnp.arange(peers, dtype=jnp.int32) ^ me
    places = [sum(((apart >> bit) & 1) << k for k, bit in enumerate(order)) for order in orders]
    place = jnp.where(core == 0, places[0], places[1])

    own_out, own_lse = own_attention(queries, keys, values.T)
    pairs = incoming[:, slots * TILE : slots * TILE + slots, 0].astype(jnp.int32)
    answers = attend_slots(
        pairs.reshape(peers * slots), incoming, prefix_keys, prefix_values.T, slots, heads
    )
    back = lax.all_to_all(answers, "ctx", split_axis=0, concat_axis=0, tiled=True)
    att = combine(owner, rank, place, back, own_out, own_lse, slots)
    att_other = lax.ppermute(att, "head", swap)
    return project(att, att_other, w_own, w_other)


def solution(mesh):
    return jax.shard_map(
        shards,
        mesh=mesh,
        in_specs=(
            P("ctx", "head"),
            P("ctx", "head"),
            P("ctx", "head"),
            P("ctx", "head"),
            P("ctx", "head"),
            P("head", "ctx", None, None),
            P("head", "ctx", None),
        ),
        out_specs=P("ctx", "head"),
        check_vma=False,
    )
```

```python
import math

import jax
import jax.numpy as jnp
from jax import lax
from jax.experimental import pallas as pl
from jax.experimental.pallas import tpu as pltpu
from jax.sharding import PartitionSpec as P


D_HEAD = 128
TILE = 128
BLOCK = 512
TOPK = 3
SCALE = D_HEAD ** (-0.5)
LOG2E = 1.4426950408889634
BF16 = jnp.bfloat16
F32 = jnp.float32


def round_up(n, m):
    return (n + m - 1) // m * m


def smem():
    return pl.BlockSpec(memory_space=pltpu.SMEM)


def route_queries(picked, queries, peers, parts, blocks_here):
    tok_rows, width = queries.shape
    heads = width // D_HEAD
    requests = picked.shape[0]
    slots = sum(parts)
    tails = [round_up(n, 16) for n in parts]
    steps = 4 if peers % 4 == 0 else 1
    per_step = peers // steps
    full = peers * slots == requests

    def body(picked_ref, q_ref, *refs):
        outs, (owner_ref, rank_ref, source, pair, count) = refs[: len(parts)], refs[len(parts) :]
        step = pl.program_id(0)

        @pl.when(step == 0)
        def _():
            for p in range(peers):
                count[p] = 0
            if not full:
                for i in range(peers * slots):
                    source[i] = -1
                    pair[i] = 0
            for r in range(requests):
                block = picked_ref[r]
                owner = block // blocks_here if blocks_here > 1 else block
                local = block % blocks_here if blocks_here > 1 else 0
                rank = count[owner]
                slot = owner * slots + rank
                source[slot] = r // TOPK
                pair[slot] = local * heads + (r // TOPK) % heads
                count[owner] = rank + 1
                owner_ref[r] = owner
                rank_ref[r] = rank

        for i in range(per_step):
            first = 0
            for n, tail, out_ref in zip(parts, tails, outs):
                sub = lax.broadcasted_iota(jnp.int32, (tail, TILE), 0)
                ids = jnp.zeros((tail, TILE), F32)
                for s in range(n):
                    slot = (step * per_step + i) * slots + first + s
                    row = source[slot]
                    safe = row if full else jnp.maximum(row, 0)
                    start = pl.multiple_of((safe // heads) * TILE, TILE)
                    lane = pl.multiple_of((safe % heads) * D_HEAD, D_HEAD)
                    q = q_ref[pl.ds(start, TILE), pl.ds(lane, D_HEAD)]
                    if not full:
                        q = jnp.where(row >= 0, q, jnp.zeros_like(q))
                    out_ref[i, s * TILE : (s + 1) * TILE, :] = q
                    ids = jnp.where(sub == s, pair[slot].astype(F32), ids)
                out_ref[i, n * TILE :, :] = ids.astype(BF16)
                first += n

    rows = [n * TILE + tail for n, tail in zip(parts, tails)]
    results = pl.pallas_call(
        body,
        grid=(steps,),
        in_specs=[smem(), pl.BlockSpec((tok_rows, width), lambda i: (0, 0))],
        out_specs=[pl.BlockSpec((per_step, n, TILE), lambda i: (i, 0, 0)) for n in rows]
        + [smem(), smem()],
        out_shape=[jax.ShapeDtypeStruct((peers, n, TILE), BF16) for n in rows]
        + [jax.ShapeDtypeStruct((requests,), jnp.int32)] * 2,
        scratch_shapes=[
            pltpu.SMEM((peers * slots,), jnp.int32),
            pltpu.SMEM((peers * slots,), jnp.int32),
            pltpu.SMEM((peers,), jnp.int32),
        ],
        name="route",
    )(picked, queries)
    return results[: len(parts)], results[-2], results[-1]


def soft(scores):
    top = jnp.max(scores, axis=0, keepdims=True)
    weights = jnp.exp2((scores - top) * (SCALE * LOG2E))
    total = jnp.sum(weights, axis=0, keepdims=True)
    return weights.astype(BF16), total, top * SCALE + jnp.log(total)


def dot_nt(a, b):
    return lax.dot_general(a, b, (((1,), (1,)), ((), ())), preferred_element_type=F32)


def attend_slots(pairs, incoming, keys, values_t, slots, heads):
    peers, rows, _ = incoming.shape
    tail = round_up(3 * slots, 16)
    out_rows = slots * TILE + tail
    blocks = keys.shape[0] // BLOCK
    group = math.gcd(peers, max(1, 6 // slots))

    def body(pair_ref, q_ref, k_ref, v_ref, out_ref):
        sub = lax.broadcasted_iota(jnp.int32, (tail, TILE), 0)
        for i in range(group):
            p = pl.program_id(0) * group + i
            logs = jnp.zeros((tail, TILE), F32)
            for s in range(slots):
                pair = pair_ref[p * slots + s]
                head = pair % heads if blocks > 1 else pair
                start = pl.multiple_of(pair // heads * BLOCK, BLOCK) if blocks > 1 else 0
                lane = pl.multiple_of(head * D_HEAD, D_HEAD)
                k = k_ref[pl.ds(start, BLOCK), pl.ds(lane, D_HEAD)]
                v = v_ref[pl.ds(lane, D_HEAD), pl.ds(start, BLOCK)]
                q = q_ref[i, s * TILE : (s + 1) * TILE, :]
                weights, total, lse = soft(dot_nt(k, q))
                out = jnp.dot(v, weights, preferred_element_type=F32) / total
                out_ref[i, s * TILE : (s + 1) * TILE, :] = out.astype(BF16)
                high = lse.astype(BF16).astype(F32)
                middle = (lse - high).astype(BF16).astype(F32)
                low = lse - high - middle
                logs = jnp.where(sub == 3 * s, high, logs)
                logs = jnp.where(sub == 3 * s + 1, middle, logs)
                logs = jnp.where(sub == 3 * s + 2, low, logs)
            out_ref[i, slots * TILE :, :] = logs.astype(BF16)

    return pl.pallas_call(
        body,
        grid=(peers // group,),
        in_specs=[
            smem(),
            pl.BlockSpec((group, rows, TILE), lambda i: (i, 0, 0)),
            pl.BlockSpec(keys.shape, lambda i: (0, 0)),
            pl.BlockSpec(values_t.shape, lambda i: (0, 0)),
        ],
        out_specs=pl.BlockSpec((group, out_rows, TILE), lambda i: (i, 0, 0)),
        out_shape=jax.ShapeDtypeStruct((peers, out_rows, TILE), BF16),
        name="attend",
    )(pairs, incoming, keys, values_t)


def own_attention(queries, keys, values, prefix_values):
    tok_rows, width = queries.shape
    heads = width // D_HEAD
    blocks = tok_rows // BLOCK

    def body(q_ref, k_ref, v_ref, pv_ref, out_ref, lse_ref, turned_ref):
        turned_ref[...] = pv_ref[...].T
        v_t = v_ref[...].T
        for t in range(BLOCK // TILE):
            seen = (t + 1) * TILE
            scores = dot_nt(k_ref[:seen, :], q_ref[t * TILE : seen, :])
            key = lax.broadcasted_iota(jnp.int32, scores.shape, 0)
            query = lax.broadcasted_iota(jnp.int32, scores.shape, 1) + t * TILE
            weights, total, lse = soft(jnp.where(key <= query, scores, -jnp.inf))
            out = jnp.dot(v_t[:, :seen], weights, preferred_element_type=F32) / total
            out_ref[:, t * TILE : seen] = out
            lse_ref[0, :, t * TILE : seen] = lse

    block = pl.BlockSpec((BLOCK, D_HEAD), lambda b, h: (b, h))
    block_t = pl.BlockSpec((D_HEAD, BLOCK), lambda b, h: (h, b))
    return pl.pallas_call(
        body,
        grid=(blocks, heads),
        in_specs=[block] * 4,
        out_specs=[block_t, pl.BlockSpec((1, 1, BLOCK), lambda b, h: (h, 0, b)), block_t],
        out_shape=[
            jax.ShapeDtypeStruct((width, tok_rows), F32),
            jax.ShapeDtypeStruct((heads, 1, tok_rows), F32),
            jax.ShapeDtypeStruct((width, tok_rows), BF16),
        ],
        name="own",
    )(queries, keys, values, prefix_values)


def combine(owner, rank, place, backs, own_out, own_lse, parts):
    peers = backs[0].shape[0]
    width, tok_rows = own_out.shape
    heads = width // D_HEAD
    tiles = tok_rows // TILE
    chunk = width // peers

    def body(owner_ref, rank_ref, place_ref, *refs):
        back_refs, (out_ref, lse_ref, att_ref, turned) = refs[: len(parts)], refs[len(parts) :]
        t = pl.program_id(0)

        def answer(r):
            p, rank = owner_ref[r], rank_ref[r]
            first, part, log = 0, None, None
            for n, back_ref in zip(parts, back_refs):
                s = jnp.clip(rank - first, 0, n - 1)
                here = back_ref[p, pl.ds(pl.multiple_of(s * TILE, TILE), TILE), :]
                terms = back_ref[p, n * TILE :, :].astype(F32)
                sub = lax.broadcasted_iota(jnp.int32, terms.shape, 0)
                mine = jnp.logical_and(sub >= 3 * s, sub < 3 * s + 3)
                here_log = jnp.sum(jnp.where(mine, terms, 0.0), axis=0, keepdims=True)
                part = here if part is None else jnp.where(rank >= first, here, part)
                log = here_log if log is None else jnp.where(rank >= first, here_log, log)
                first += n
            return part.astype(F32), log

        for h in range(heads):
            logs, pieces = [lse_ref[h]], [out_ref[h * D_HEAD : (h + 1) * D_HEAD, :]]
            for j in range(TOPK):
                piece, log = answer((t * heads + h) * TOPK + j)
                pieces.append(piece)
                logs.append(log)
            top = logs[0]
            for log in logs[1:]:
                top = jnp.maximum(top, log)
            factors = [jnp.exp(log - top) for log in logs]
            total = factors[0]
            for factor in factors[1:]:
                total = total + factor
            inverse = 1.0 / total
            mixed = pieces[0] * (factors[0] * inverse)
            for factor, piece in zip(factors[1:], pieces[1:]):
                mixed = mixed + piece * (factor * inverse)
            for i in range(D_HEAD // chunk):
                at = pl.multiple_of(place_ref[h * (D_HEAD // chunk) + i] * chunk, chunk)
                turned[pl.ds(at, chunk), :] = mixed[i * chunk : (i + 1) * chunk, :]
        for h in range(heads):
            lanes = slice(h * D_HEAD, (h + 1) * D_HEAD)
            att_ref[:, lanes] = turned[lanes, :].T.astype(BF16)

    return pl.pallas_call(
        body,
        grid=(tiles,),
        in_specs=[smem(), smem(), smem()]
        + [pl.BlockSpec(back.shape, lambda i: (0, 0, 0)) for back in backs]
        + [
            pl.BlockSpec((width, TILE), lambda i: (0, i)),
            pl.BlockSpec((heads, 1, TILE), lambda i: (0, 0, i)),
        ],
        out_specs=pl.BlockSpec((TILE, width), lambda i: (i, 0)),
        out_shape=jax.ShapeDtypeStruct((tok_rows, width), BF16),
        scratch_shapes=[pltpu.VMEM((width, TILE), F32)],
        name="combine",
    )(owner, rank, place, *backs, own_out, own_lse)


def project(att_own, att_other, weights):
    rows, depth = att_own.shape
    piece, width = weights[0].shape
    part = min(width, 512)

    def body(a_ref, b_ref, w0, w1, w2, w3, out_ref):
        total = jnp.dot(a_ref[:, :piece], w0[...], preferred_element_type=F32)
        total += jnp.dot(a_ref[:, piece:], w1[...], preferred_element_type=F32)
        total += jnp.dot(b_ref[:, :piece], w2[...], preferred_element_type=F32)
        total += jnp.dot(b_ref[:, piece:], w3[...], preferred_element_type=F32)
        out_ref[...] = total.astype(BF16)

    held = pl.BlockSpec((rows, depth), lambda i: (0, 0))
    weight = pl.BlockSpec((piece, part), lambda i: (0, i))
    return pl.pallas_call(
        body,
        grid=(width // part,),
        in_specs=[held, held] + [weight] * 4,
        out_specs=pl.BlockSpec((rows, part), lambda i: (0, i)),
        out_shape=jax.ShapeDtypeStruct((rows, width), BF16),
        name="project",
    )(att_own, att_other, *weights)


def bit_orders(peers):
    bits = int(math.log2(peers))
    high = list(range(bits - 1, 2, -1))
    return [high + [2, 1, 0], high + [2, 0, 1]]


def doubling_pairs(peers, orders, step, crossed=False):
    pairs = []
    for c in range(peers):
        for h in range(2):
            pairs.append((2 * c + h, 2 * (c ^ (1 << orders[h][step])) + (1 - h if crossed else h)))
    return pairs


def joined(a, b):
    return lax.optimization_barrier(jnp.concatenate([a, b], axis=0))


def shards(queries, keys, values, prefix_keys, prefix_values, selected, out_weight):
    tok_rows, width = queries.shape
    heads = width // D_HEAD
    tiles = tok_rows // TILE
    blocks_here = prefix_keys.shape[0] // BLOCK
    peers = lax.axis_size("ctx")
    me, core = lax.axis_index("ctx"), lax.axis_index("head")
    requests = tiles * heads * TOPK
    capacity = -(-requests // (peers * blocks_here))
    slots = capacity * blocks_here
    swap = [(0, 1), (1, 0)]
    both = ("ctx", "head")

    orders = bit_orders(peers)
    steps = len(orders[0])
    weight = out_weight[0]
    for step in range(steps - 1):
        got = lax.ppermute(weight, both, doubling_pairs(peers, orders, step))
        weight = joined(weight, got)
    half = weight.shape[1] // 2
    mine = lax.dynamic_slice_in_dim(weight, core * half, half, 1)
    theirs = lax.dynamic_slice_in_dim(weight, (1 - core) * half, half, 1)
    mine, theirs = lax.optimization_barrier((mine, theirs))
    far_own = lax.ppermute(mine, both, doubling_pairs(peers, orders, steps - 1))
    far_other = lax.ppermute(theirs, both, doubling_pairs(peers, orders, steps - 1, True))
    near_other = lax.ppermute(theirs, "head", swap)

    parts = [slots]
    outgoing, owner, rank = route_queries(
        selected.reshape(requests), queries, peers, parts, blocks_here
    )
    incoming = []
    for sent in outgoing:
        incoming.append(lax.all_to_all(sent, "ctx", split_axis=0, concat_axis=0, tiled=True))
    own_out, own_lse, turned = own_attention(queries, keys, values, prefix_values)

    apart = jnp.arange(peers, dtype=jnp.int32) ^ me
    places = [sum(((apart >> bit) & 1) << k for k, bit in enumerate(order)) for order in orders]
    place = jnp.where(core == 0, places[0], places[1])

    backs = []
    for n, asked in zip(parts, incoming):
        pairs = asked[:, n * TILE : n * TILE + n, 0].astype(jnp.int32).reshape(peers * n)
        answers = attend_slots(pairs, asked, prefix_keys, turned, n, heads)
        backs.append(lax.all_to_all(answers, "ctx", split_axis=0, concat_axis=0, tiled=True))
    att = combine(owner, rank, place, backs, own_out, own_lse, parts)
    att_other = lax.ppermute(att, "head", swap)
    return project(att, att_other, (mine, far_own, near_other, far_other))


def solution(mesh):
    return jax.shard_map(
        shards,
        mesh=mesh,
        in_specs=(
            P("ctx", "head"),
            P("ctx", "head"),
            P("ctx", "head"),
            P("ctx", "head"),
            P("ctx", "head"),
            P("head", "ctx", None, None),
            P("head", "ctx", None),
        ),
        out_specs=P("ctx", "head"),
        check_vma=False,
    )
```

```python
import math

import jax
import jax.numpy as jnp
from jax import lax
from jax.experimental import pallas as pl
from jax.experimental.pallas import tpu as pltpu
from jax.sharding import PartitionSpec as P


D_HEAD = 128
TILE = 128
BLOCK = 512
TOPK = 3
UNROLL = 24
SCALE = D_HEAD ** (-0.5)
LOG2E = 1.4426950408889634
BF16 = jnp.bfloat16
F32 = jnp.float32


def round_up(n, m):
    return (n + m - 1) // m * m


def smem():
    return pl.BlockSpec(memory_space=pltpu.SMEM)


def route_queries(picked, queries, peers, parts, blocks_here):
    tok_rows, width = queries.shape
    heads = width // D_HEAD
    requests = picked.shape[0]
    slots = sum(parts)
    tails = [round_up(n, 16) for n in parts]
    steps = 4 if peers % 4 == 0 else 1
    per_step = peers // steps
    full = peers * slots == requests

    def body(picked_ref, q_ref, *refs):
        outs, (owner_ref, rank_ref, source, pair, count) = refs[: len(parts)], refs[len(parts) :]
        step = pl.program_id(0)

        @pl.when(step == 0)
        def _():
            for p in range(peers):
                count[p] = 0
            if not full:
                for i in range(peers * slots):
                    source[i] = -1
                    pair[i] = 0
            for r in range(requests):
                block = picked_ref[r]
                owner = block // blocks_here if blocks_here > 1 else block
                local = block % blocks_here if blocks_here > 1 else 0
                rank = count[owner]
                slot = owner * slots + rank
                source[slot] = r // TOPK
                pair[slot] = local * heads + (r // TOPK) % heads
                count[owner] = rank + 1
                owner_ref[r] = owner
                rank_ref[r] = rank

        for i in range(per_step):
            first = 0
            for n, tail, out_ref in zip(parts, tails, outs):
                sub = lax.broadcasted_iota(jnp.int32, (tail, TILE), 0)
                ids = jnp.zeros((tail, TILE), F32)
                for s in range(n):
                    slot = (step * per_step + i) * slots + first + s
                    row = source[slot]
                    safe = row if full else jnp.maximum(row, 0)
                    start = pl.multiple_of((safe // heads) * TILE, TILE)
                    lane = pl.multiple_of((safe % heads) * D_HEAD, D_HEAD)
                    q = q_ref[pl.ds(start, TILE), pl.ds(lane, D_HEAD)]
                    if not full:
                        q = jnp.where(row >= 0, q, jnp.zeros_like(q))
                    out_ref[i, s * TILE : (s + 1) * TILE, :] = q
                    ids = jnp.where(sub == s, pair[slot].astype(F32), ids)
                out_ref[i, n * TILE :, :] = ids.astype(BF16)
                first += n

    rows = [n * TILE + tail for n, tail in zip(parts, tails)]
    results = pl.pallas_call(
        body,
        grid=(steps,),
        in_specs=[smem(), pl.BlockSpec((tok_rows, width), lambda i: (0, 0))],
        out_specs=[pl.BlockSpec((per_step, n, TILE), lambda i: (i, 0, 0)) for n in rows]
        + [smem(), smem()],
        out_shape=[jax.ShapeDtypeStruct((peers, n, TILE), BF16) for n in rows]
        + [jax.ShapeDtypeStruct((requests,), jnp.int32)] * 2,
        scratch_shapes=[
            pltpu.SMEM((peers * slots,), jnp.int32),
            pltpu.SMEM((peers * slots,), jnp.int32),
            pltpu.SMEM((peers,), jnp.int32),
        ],
        name="route",
    )(picked, queries)
    return results[: len(parts)], results[-2], results[-1]


def soft(scores):
    top = jnp.max(scores, axis=0, keepdims=True)
    weights = jnp.exp2((scores - top) * (SCALE * LOG2E))
    total = jnp.sum(weights, axis=0, keepdims=True)
    return weights.astype(BF16), total, top * SCALE + jnp.log(total)


def dot_nt(a, b):
    return lax.dot_general(a, b, (((1,), (1,)), ((), ())), preferred_element_type=F32)


def attend_slots(pairs, incoming, keys, values_t, slots, heads):
    peers, rows, _ = incoming.shape
    tail = round_up(3 * slots, 16)
    out_rows = slots * TILE + tail
    blocks = keys.shape[0] // BLOCK
    group = math.gcd(peers, max(1, UNROLL // slots))

    def body(pair_ref, q_ref, k_ref, v_ref, out_ref):
        sub = lax.broadcasted_iota(jnp.int32, (tail, TILE), 0)
        for i in range(group):
            p = pl.program_id(0) * group + i
            logs = jnp.zeros((tail, TILE), F32)
            for s in range(slots):
                pair = pair_ref[p * slots + s]
                head = pair % heads if blocks > 1 else pair
                start = pl.multiple_of(pair // heads * BLOCK, BLOCK) if blocks > 1 else 0
                lane = pl.multiple_of(head * D_HEAD, D_HEAD)
                k = k_ref[pl.ds(start, BLOCK), pl.ds(lane, D_HEAD)]
                v = v_ref[pl.ds(lane, D_HEAD), pl.ds(start, BLOCK)]
                q = q_ref[i, s * TILE : (s + 1) * TILE, :]
                weights, total, lse = soft(dot_nt(k, q))
                out = jnp.dot(v, weights, preferred_element_type=F32) / total
                out_ref[i, s * TILE : (s + 1) * TILE, :] = out.astype(BF16)
                high = lse.astype(BF16).astype(F32)
                middle = (lse - high).astype(BF16).astype(F32)
                low = lse - high - middle
                logs = jnp.where(sub == 3 * s, high, logs)
                logs = jnp.where(sub == 3 * s + 1, middle, logs)
                logs = jnp.where(sub == 3 * s + 2, low, logs)
            out_ref[i, slots * TILE :, :] = logs.astype(BF16)

    return pl.pallas_call(
        body,
        grid=(peers // group,),
        in_specs=[
            smem(),
            pl.BlockSpec((group, rows, TILE), lambda i: (i, 0, 0)),
            pl.BlockSpec(keys.shape, lambda i: (0, 0)),
            pl.BlockSpec(values_t.shape, lambda i: (0, 0)),
        ],
        out_specs=pl.BlockSpec((group, out_rows, TILE), lambda i: (i, 0, 0)),
        out_shape=jax.ShapeDtypeStruct((peers, out_rows, TILE), BF16),
        name="attend",
    )(pairs, incoming, keys, values_t)


def own_attention(queries, keys, values, prefix_values):
    tok_rows, width = queries.shape
    heads = width // D_HEAD
    blocks = tok_rows // BLOCK

    def body(q_ref, k_ref, v_ref, pv_ref, out_ref, lse_ref, turned_ref):
        turned_ref[...] = pv_ref[...].T
        v_t = v_ref[...].T
        for t in range(BLOCK // TILE):
            seen = (t + 1) * TILE
            scores = dot_nt(k_ref[:seen, :], q_ref[t * TILE : seen, :])
            key = lax.broadcasted_iota(jnp.int32, scores.shape, 0)
            query = lax.broadcasted_iota(jnp.int32, scores.shape, 1) + t * TILE
            weights, total, lse = soft(jnp.where(key <= query, scores, -jnp.inf))
            out = jnp.dot(v_t[:, :seen], weights, preferred_element_type=F32) / total
            out_ref[:, t * TILE : seen] = out
            lse_ref[0, :, t * TILE : seen] = lse

    block = pl.BlockSpec((BLOCK, D_HEAD), lambda b, h: (b, h))
    block_t = pl.BlockSpec((D_HEAD, BLOCK), lambda b, h: (h, b))
    return pl.pallas_call(
        body,
        grid=(blocks, heads),
        in_specs=[block] * 4,
        out_specs=[block_t, pl.BlockSpec((1, 1, BLOCK), lambda b, h: (h, 0, b)), block_t],
        out_shape=[
            jax.ShapeDtypeStruct((width, tok_rows), F32),
            jax.ShapeDtypeStruct((heads, 1, tok_rows), F32),
            jax.ShapeDtypeStruct((width, tok_rows), BF16),
        ],
        name="own",
    )(queries, keys, values, prefix_values)


def combine(owner, rank, place, backs, own_out, own_lse, parts):
    peers = backs[0].shape[0]
    width, tok_rows = own_out.shape
    heads = width // D_HEAD
    tiles = tok_rows // TILE
    chunk = width // peers

    def body(owner_ref, rank_ref, place_ref, *refs):
        back_refs, (out_ref, lse_ref, att_ref, turned) = refs[: len(parts)], refs[len(parts) :]
        t = pl.program_id(0)

        def answer(r):
            p, rank = owner_ref[r], rank_ref[r]
            first, part, log = 0, None, None
            for n, back_ref in zip(parts, back_refs):
                s = jnp.clip(rank - first, 0, n - 1)
                here = back_ref[p, pl.ds(pl.multiple_of(s * TILE, TILE), TILE), :]
                terms = back_ref[p, n * TILE :, :].astype(F32)
                sub = lax.broadcasted_iota(jnp.int32, terms.shape, 0)
                mine = jnp.logical_and(sub >= 3 * s, sub < 3 * s + 3)
                here_log = jnp.sum(jnp.where(mine, terms, 0.0), axis=0, keepdims=True)
                part = here if part is None else jnp.where(rank >= first, here, part)
                log = here_log if log is None else jnp.where(rank >= first, here_log, log)
                first += n
            return part.astype(F32), log

        for h in range(heads):
            logs, pieces = [lse_ref[h]], [out_ref[h * D_HEAD : (h + 1) * D_HEAD, :]]
            for j in range(TOPK):
                piece, log = answer((t * heads + h) * TOPK + j)
                pieces.append(piece)
                logs.append(log)
            top = logs[0]
            for log in logs[1:]:
                top = jnp.maximum(top, log)
            factors = [jnp.exp(log - top) for log in logs]
            total = factors[0]
            for factor in factors[1:]:
                total = total + factor
            inverse = 1.0 / total
            mixed = pieces[0] * (factors[0] * inverse)
            for factor, piece in zip(factors[1:], pieces[1:]):
                mixed = mixed + piece * (factor * inverse)
            for i in range(D_HEAD // chunk):
                at = pl.multiple_of(place_ref[h * (D_HEAD // chunk) + i] * chunk, chunk)
                turned[pl.ds(at, chunk), :] = mixed[i * chunk : (i + 1) * chunk, :]
        for h in range(heads):
            lanes = slice(h * D_HEAD, (h + 1) * D_HEAD)
            att_ref[:, lanes] = turned[lanes, :].T.astype(BF16)

    return pl.pallas_call(
        body,
        grid=(tiles,),
        in_specs=[smem(), smem(), smem()]
        + [pl.BlockSpec(back.shape, lambda i: (0, 0, 0)) for back in backs]
        + [
            pl.BlockSpec((width, TILE), lambda i: (0, i)),
            pl.BlockSpec((heads, 1, TILE), lambda i: (0, 0, i)),
        ],
        out_specs=pl.BlockSpec((TILE, width), lambda i: (i, 0)),
        out_shape=jax.ShapeDtypeStruct((tok_rows, width), BF16),
        scratch_shapes=[pltpu.VMEM((width, TILE), F32)],
        name="combine",
    )(owner, rank, place, *backs, own_out, own_lse)


def project(att_own, att_other, halves):
    rows, depth = att_own.shape
    piece, columns = halves[0][0].shape
    part = min(columns, 1024)
    count = columns // part

    def body(a_ref, b_ref, *refs):
        out_ref = refs[-1]
        for i in range(len(halves)):
            w0, w1, w2, w3 = refs[4 * i : 4 * i + 4]

            @pl.when(pl.program_id(0) // count == i)
            def _():
                total = jnp.dot(a_ref[:, :piece], w0[...], preferred_element_type=F32)
                total += jnp.dot(a_ref[:, piece:], w1[...], preferred_element_type=F32)
                total += jnp.dot(b_ref[:, :piece], w2[...], preferred_element_type=F32)
                total += jnp.dot(b_ref[:, piece:], w3[...], preferred_element_type=F32)
                out_ref[...] = total.astype(BF16)

    def weight(i):
        return pl.BlockSpec((piece, part), lambda n: (0, jnp.clip(n - i * count, 0, count - 1)))

    held = pl.BlockSpec((rows, depth), lambda n: (0, 0))
    return pl.pallas_call(
        body,
        grid=(len(halves) * count,),
        in_specs=[held, held] + [weight(i) for i in range(len(halves)) for _ in range(4)],
        out_specs=pl.BlockSpec((rows, part), lambda n: (0, n)),
        out_shape=jax.ShapeDtypeStruct((rows, len(halves) * columns), BF16),
        name="project",
    )(att_own, att_other, *[w for half in halves for w in half])


def bit_orders(peers):
    bits = int(math.log2(peers))
    high = list(range(bits - 1, 2, -1))
    return [high + [2, 1, 0], high + [2, 0, 1]]


def doubling_pairs(peers, orders, step, crossed=False):
    pairs = []
    for c in range(peers):
        for h in range(2):
            pairs.append((2 * c + h, 2 * (c ^ (1 << orders[h][step])) + (1 - h if crossed else h)))
    return pairs


def joined(a, b):
    return lax.optimization_barrier(jnp.concatenate([a, b], axis=0))


def stacked_halves(pieces, core):
    rows, width = pieces[0].shape
    half, count = width // 2, len(pieces)
    step = rows // 4 if rows % 64 == 0 else rows

    def body(core_ref, *refs):
        mine_ref, theirs_ref = refs[2 * count :]
        for i in range(count):
            mine_ref[i], theirs_ref[i] = refs[i][...], refs[count + i][...]

    mine = pl.BlockSpec((step, half), lambda i, core_ref: (i, core_ref[0]))
    theirs = pl.BlockSpec((step, half), lambda i, core_ref: (i, 1 - core_ref[0]))
    out = pl.BlockSpec((count, step, half), lambda i, core_ref: (0, i, 0))
    results = pl.pallas_call(
        body,
        grid_spec=pltpu.PrefetchScalarGridSpec(
            num_scalar_prefetch=1,
            grid=(rows // step,),
            in_specs=[mine] * count + [theirs] * count,
            out_specs=[out, out],
        ),
        out_shape=[jax.ShapeDtypeStruct((count, rows, half), pieces[0].dtype)] * 2,
        name="halves",
    )(core.reshape(1), *pieces, *pieces)
    return [result.reshape(count * rows, half) for result in results]


def shards(queries, keys, values, prefix_keys, prefix_values, selected, out_weight):
    tok_rows, width = queries.shape
    heads = width // D_HEAD
    tiles = tok_rows // TILE
    blocks_here = prefix_keys.shape[0] // BLOCK
    peers = lax.axis_size("ctx")
    me, core = lax.axis_index("ctx"), lax.axis_index("head")
    requests = tiles * heads * TOPK
    capacity = -(-requests // (peers * blocks_here))
    slots = capacity * blocks_here
    swap = [(0, 1), (1, 0)]
    both = ("ctx", "head")

    orders = bit_orders(peers)
    steps = len(orders[0])

    def gathered(weight):
        for step in range(steps - 3):
            got = lax.ppermute(weight, both, doubling_pairs(peers, orders, step))
            weight = joined(weight, got)
        pieces = [weight]
        for step in range(steps - 3, steps - 1):
            pairs = doubling_pairs(peers, orders, step)
            pieces += [lax.ppermute(piece, both, pairs) for piece in pieces]
        mine, theirs = stacked_halves(pieces, core)
        far_own = lax.ppermute(mine, both, doubling_pairs(peers, orders, steps - 1))
        far_other = lax.ppermute(theirs, both, doubling_pairs(peers, orders, steps - 1, True))
        near_other = lax.ppermute(theirs, "head", swap)
        return mine, far_own, near_other, far_other

    weights = [gathered(out_weight[0])]

    parts = [slots]
    outgoing, owner, rank = route_queries(
        selected.reshape(requests), queries, peers, parts, blocks_here
    )
    incoming = []
    for sent in outgoing:
        incoming.append(lax.all_to_all(sent, "ctx", split_axis=0, concat_axis=0, tiled=True))
    own_out, own_lse, turned = own_attention(queries, keys, values, prefix_values)

    apart = jnp.arange(peers, dtype=jnp.int32) ^ me
    places = [sum(((apart >> bit) & 1) << k for k, bit in enumerate(order)) for order in orders]
    place = jnp.where(core == 0, places[0], places[1])

    backs = []
    for n, asked in zip(parts, incoming):
        pairs = asked[:, n * TILE : n * TILE + n, 0].astype(jnp.int32).reshape(peers * n)
        answers = attend_slots(pairs, asked, prefix_keys, turned, n, heads)
        backs.append(lax.all_to_all(answers, "ctx", split_axis=0, concat_axis=0, tiled=True))
    att = combine(owner, rank, place, backs, own_out, own_lse, parts)
    att_other = lax.ppermute(att, "head", swap)
    return project(att, att_other, weights)


def solution(mesh):
    return jax.shard_map(
        shards,
        mesh=mesh,
        in_specs=(
            P("ctx", "head"),
            P("ctx", "head"),
            P("ctx", "head"),
            P("ctx", "head"),
            P("ctx", "head"),
            P("head", "ctx", None, None),
            P("head", "ctx", None),
        ),
        out_specs=P("ctx", "head"),
        check_vma=False,
    )
```

```python
import math

import jax
import jax.numpy as jnp
from jax import lax
from jax.experimental import pallas as pl
from jax.experimental.pallas import tpu as pltpu
from jax.sharding import PartitionSpec as P


D_HEAD = 128
TILE = 128
BLOCK = 512
TOPK = 3
UNROLL = 48
SCALE = D_HEAD ** (-0.5)
LOG2E = 1.4426950408889634
BF16 = jnp.bfloat16
F32 = jnp.float32


def round_up(n, m):
    return (n + m - 1) // m * m


def smem():
    return pl.BlockSpec(memory_space=pltpu.SMEM)


def route_queries(picked, queries, peers, parts, blocks_here):
    tok_rows, width = queries.shape
    heads = width // D_HEAD
    requests = picked.shape[0]
    slots = sum(parts)
    tails = [round_up(n, 16) for n in parts]
    steps = math.gcd(peers, 2)
    per_step = peers // steps
    full = peers * slots == requests

    def body(picked_ref, q_ref, *refs):
        outs, (owner_ref, rank_ref, source, pair, count) = refs[: len(parts)], refs[len(parts) :]
        step = pl.program_id(0)

        @pl.when(step == 0)
        def _():
            for p in range(peers):
                count[p] = 0
            if not full:
                for i in range(peers * slots):
                    source[i] = -1
                    pair[i] = 0
            for r in range(requests):
                block = picked_ref[r]
                owner = block // blocks_here if blocks_here > 1 else block
                local = block % blocks_here if blocks_here > 1 else 0
                rank = count[owner]
                slot = owner * slots + rank
                source[slot] = r // TOPK
                pair[slot] = local * heads + (r // TOPK) % heads
                count[owner] = rank + 1
                owner_ref[r] = owner
                rank_ref[r] = rank

        for i in range(per_step):
            first = 0
            for n, tail, out_ref in zip(parts, tails, outs):
                sub = lax.broadcasted_iota(jnp.int32, (tail, TILE), 0)
                ids = jnp.zeros((tail, TILE), F32)
                for s in range(n):
                    slot = (step * per_step + i) * slots + first + s
                    row = source[slot]
                    safe = row if full else jnp.maximum(row, 0)
                    start = pl.multiple_of((safe // heads) * TILE, TILE)
                    lane = pl.multiple_of((safe % heads) * D_HEAD, D_HEAD)
                    q = q_ref[pl.ds(start, TILE), pl.ds(lane, D_HEAD)]
                    if not full:
                        q = jnp.where(row >= 0, q, jnp.zeros_like(q))
                    out_ref[i, s * TILE : (s + 1) * TILE, :] = q
                    ids = jnp.where(sub == s, pair[slot].astype(F32), ids)
                out_ref[i, n * TILE :, :] = ids.astype(BF16)
                first += n

    rows = [n * TILE + tail for n, tail in zip(parts, tails)]
    results = pl.pallas_call(
        body,
        grid=(steps,),
        in_specs=[smem(), pl.BlockSpec((tok_rows, width), lambda i: (0, 0))],
        out_specs=[pl.BlockSpec((per_step, n, TILE), lambda i: (i, 0, 0)) for n in rows]
        + [smem(), smem()],
        out_shape=[jax.ShapeDtypeStruct((peers, n, TILE), BF16) for n in rows]
        + [jax.ShapeDtypeStruct((requests,), jnp.int32)] * 2,
        scratch_shapes=[
            pltpu.SMEM((peers * slots,), jnp.int32),
            pltpu.SMEM((peers * slots,), jnp.int32),
            pltpu.SMEM((peers,), jnp.int32),
        ],
        name="route",
    )(picked, queries)
    return results[: len(parts)], results[-2], results[-1]


def soft(scores):
    top = jnp.max(scores, axis=0, keepdims=True)
    weights = jnp.exp2((scores - top) * (SCALE * LOG2E))
    total = jnp.sum(weights, axis=0, keepdims=True)
    return weights.astype(BF16), total, top * SCALE + jnp.log(total)


def dot_nt(a, b):
    return lax.dot_general(a, b, (((1,), (1,)), ((), ())), preferred_element_type=F32)


def attend_slots(pairs, incoming, keys, values_t, slots, heads):
    peers, rows, _ = incoming.shape
    tail = round_up(3 * slots, 16)
    out_rows = slots * TILE + tail
    blocks = keys.shape[0] // BLOCK
    group = math.gcd(peers, max(1, UNROLL // slots))

    def body(pair_ref, q_ref, k_ref, v_ref, out_ref):
        sub = lax.broadcasted_iota(jnp.int32, (tail, TILE), 0)
        for i in range(group):
            p = pl.program_id(0) * group + i
            logs = jnp.zeros((tail, TILE), F32)
            for s in range(slots):
                pair = pair_ref[p * slots + s]
                head = pair % heads if blocks > 1 else pair
                start = pl.multiple_of(pair // heads * BLOCK, BLOCK) if blocks > 1 else 0
                lane = pl.multiple_of(head * D_HEAD, D_HEAD)
                k = k_ref[pl.ds(start, BLOCK), pl.ds(lane, D_HEAD)]
                v = v_ref[pl.ds(lane, D_HEAD), pl.ds(start, BLOCK)]
                q = q_ref[i, s * TILE : (s + 1) * TILE, :]
                weights, total, lse = soft(dot_nt(k, q))
                out = jnp.dot(v, weights, preferred_element_type=F32) / total
                out_ref[i, s * TILE : (s + 1) * TILE, :] = out.astype(BF16)
                high = lse.astype(BF16).astype(F32)
                middle = (lse - high).astype(BF16).astype(F32)
                low = lse - high - middle
                logs = jnp.where(sub == 3 * s, high, logs)
                logs = jnp.where(sub == 3 * s + 1, middle, logs)
                logs = jnp.where(sub == 3 * s + 2, low, logs)
            out_ref[i, slots * TILE :, :] = logs.astype(BF16)

    return pl.pallas_call(
        body,
        grid=(peers // group,),
        in_specs=[
            smem(),
            pl.BlockSpec((group, rows, TILE), lambda i: (i, 0, 0)),
            pl.BlockSpec(keys.shape, lambda i: (0, 0)),
            pl.BlockSpec(values_t.shape, lambda i: (0, 0)),
        ],
        out_specs=pl.BlockSpec((group, out_rows, TILE), lambda i: (i, 0, 0)),
        out_shape=jax.ShapeDtypeStruct((peers, out_rows, TILE), BF16),
        name="attend",
    )(pairs, incoming, keys, values_t)


def own_attention(queries, keys, values, prefix_values):
    tok_rows, width = queries.shape
    heads = width // D_HEAD
    blocks = tok_rows // BLOCK

    def body(q_ref, k_ref, v_ref, pv_ref, out_ref, lse_ref, turned_ref):
        turned_ref[...] = pv_ref[...].T
        v_t = v_ref[...].T
        for t in range(BLOCK // TILE):
            seen = (t + 1) * TILE
            scores = dot_nt(k_ref[:seen, :], q_ref[t * TILE : seen, :])
            key = lax.broadcasted_iota(jnp.int32, scores.shape, 0)
            query = lax.broadcasted_iota(jnp.int32, scores.shape, 1) + t * TILE
            weights, total, lse = soft(jnp.where(key <= query, scores, -jnp.inf))
            out = jnp.dot(v_t[:, :seen], weights, preferred_element_type=F32) / total
            out_ref[:, t * TILE : seen] = out
            lse_ref[0, :, t * TILE : seen] = lse

    block = pl.BlockSpec((BLOCK, D_HEAD), lambda b, h: (b, h))
    block_t = pl.BlockSpec((D_HEAD, BLOCK), lambda b, h: (h, b))
    return pl.pallas_call(
        body,
        grid=(blocks, heads),
        in_specs=[block] * 4,
        out_specs=[block_t, pl.BlockSpec((1, 1, BLOCK), lambda b, h: (h, 0, b)), block_t],
        out_shape=[
            jax.ShapeDtypeStruct((width, tok_rows), F32),
            jax.ShapeDtypeStruct((heads, 1, tok_rows), F32),
            jax.ShapeDtypeStruct((width, tok_rows), BF16),
        ],
        name="own",
    )(queries, keys, values, prefix_values)


def combine(owner, rank, place, backs, own_out, own_lse, parts):
    peers = backs[0].shape[0]
    width, tok_rows = own_out.shape
    heads = width // D_HEAD
    tiles = tok_rows // TILE
    chunk = width // peers
    group = math.gcd(tiles, 2)

    def body(owner_ref, rank_ref, place_ref, *refs):
        back_refs, (out_ref, lse_ref, att_ref, turned) = refs[: len(parts)], refs[len(parts) :]

        def answer(r):
            p, rank = owner_ref[r], rank_ref[r]
            first, part, log = 0, None, None
            for n, back_ref in zip(parts, back_refs):
                s = jnp.clip(rank - first, 0, n - 1)
                here = back_ref[p, pl.ds(pl.multiple_of(s * TILE, TILE), TILE), :]
                terms = back_ref[p, n * TILE :, :].astype(F32)
                sub = lax.broadcasted_iota(jnp.int32, terms.shape, 0)
                mine = jnp.logical_and(sub >= 3 * s, sub < 3 * s + 3)
                here_log = jnp.sum(jnp.where(mine, terms, 0.0), axis=0, keepdims=True)
                part = here if part is None else jnp.where(rank >= first, here, part)
                log = here_log if log is None else jnp.where(rank >= first, here_log, log)
                first += n
            return part.astype(F32), log

        for i in range(group):
            t = pl.program_id(0) * group + i
            cols = slice(i * TILE, (i + 1) * TILE)
            for h in range(heads):
                logs = [lse_ref[h, :, cols]]
                pieces = [out_ref[h * D_HEAD : (h + 1) * D_HEAD, cols]]
                for j in range(TOPK):
                    piece, log = answer((t * heads + h) * TOPK + j)
                    pieces.append(piece)
                    logs.append(log)
                top = logs[0]
                for log in logs[1:]:
                    top = jnp.maximum(top, log)
                factors = [jnp.exp(log - top) for log in logs]
                total = factors[0]
                for factor in factors[1:]:
                    total = total + factor
                inverse = 1.0 / total
                mixed = pieces[0] * (factors[0] * inverse)
                for factor, piece in zip(factors[1:], pieces[1:]):
                    mixed = mixed + piece * (factor * inverse)
                for c in range(D_HEAD // chunk):
                    at = pl.multiple_of(place_ref[h * (D_HEAD // chunk) + c] * chunk, chunk)
                    turned[pl.ds(at, chunk), cols] = mixed[c * chunk : (c + 1) * chunk, :]
            for h in range(heads):
                lanes = slice(h * D_HEAD, (h + 1) * D_HEAD)
                att_ref[cols, lanes] = turned[lanes, cols].T.astype(BF16)

    return pl.pallas_call(
        body,
        grid=(tiles // group,),
        in_specs=[smem(), smem(), smem()]
        + [pl.BlockSpec(back.shape, lambda i: (0, 0, 0)) for back in backs]
        + [
            pl.BlockSpec((width, group * TILE), lambda i: (0, i)),
            pl.BlockSpec((heads, 1, group * TILE), lambda i: (0, 0, i)),
        ],
        out_specs=pl.BlockSpec((group * TILE, width), lambda i: (i, 0)),
        out_shape=jax.ShapeDtypeStruct((tok_rows, width), BF16),
        scratch_shapes=[pltpu.VMEM((width, group * TILE), F32)],
        name="combine",
    )(owner, rank, place, *backs, own_out, own_lse)


def project(att_own, att_other, halves):
    rows, depth = att_own.shape
    piece, columns = halves[0][0].shape
    part = min(columns, 1024)
    count = columns // part

    def body(a_ref, b_ref, *refs):
        out_ref = refs[-1]
        for i in range(len(halves)):
            w0, w1, w2, w3 = refs[4 * i : 4 * i + 4]

            @pl.when(pl.program_id(0) // count == i)
            def _():
                total = jnp.dot(a_ref[:, :piece], w0[...], preferred_element_type=F32)
                total += jnp.dot(a_ref[:, piece:], w1[...], preferred_element_type=F32)
                total += jnp.dot(b_ref[:, :piece], w2[...], preferred_element_type=F32)
                total += jnp.dot(b_ref[:, piece:], w3[...], preferred_element_type=F32)
                out_ref[...] = total.astype(BF16)

    def weight(i):
        return pl.BlockSpec((piece, part), lambda n: (0, jnp.clip(n - i * count, 0, count - 1)))

    held = pl.BlockSpec((rows, depth), lambda n: (0, 0))
    return pl.pallas_call(
        body,
        grid=(len(halves) * count,),
        in_specs=[held, held] + [weight(i) for i in range(len(halves)) for _ in range(4)],
        out_specs=pl.BlockSpec((rows, part), lambda n: (0, n)),
        out_shape=jax.ShapeDtypeStruct((rows, len(halves) * columns), BF16),
        name="project",
    )(att_own, att_other, *[w for half in halves for w in half])


def bit_orders(peers):
    bits = int(math.log2(peers))
    high = list(range(bits - 1, 2, -1))
    return [high + [2, 1, 0], high + [2, 0, 1]]


def doubling_pairs(peers, orders, step, crossed=False):
    pairs = []
    for c in range(peers):
        for h in range(2):
            pairs.append((2 * c + h, 2 * (c ^ (1 << orders[h][step])) + (1 - h if crossed else h)))
    return pairs


def joined(a, b):
    return lax.optimization_barrier(jnp.concatenate([a, b], axis=0))


def stacked_halves(pieces, core):
    rows, width = pieces[0].shape
    half, count = width // 2, len(pieces)
    step = rows // 4 if rows % 64 == 0 else rows

    def body(core_ref, *refs):
        mine_ref, theirs_ref = refs[2 * count :]
        for i in range(count):
            mine_ref[i], theirs_ref[i] = refs[i][...], refs[count + i][...]

    mine = pl.BlockSpec((step, half), lambda i, core_ref: (i, core_ref[0]))
    theirs = pl.BlockSpec((step, half), lambda i, core_ref: (i, 1 - core_ref[0]))
    out = pl.BlockSpec((count, step, half), lambda i, core_ref: (0, i, 0))
    results = pl.pallas_call(
        body,
        grid_spec=pltpu.PrefetchScalarGridSpec(
            num_scalar_prefetch=1,
            grid=(rows // step,),
            in_specs=[mine] * count + [theirs] * count,
            out_specs=[out, out],
        ),
        out_shape=[jax.ShapeDtypeStruct((count, rows, half), pieces[0].dtype)] * 2,
        name="halves",
    )(core.reshape(1), *pieces, *pieces)
    return [result.reshape(count * rows, half) for result in results]


def shards(queries, keys, values, prefix_keys, prefix_values, selected, out_weight):
    tok_rows, width = queries.shape
    heads = width // D_HEAD
    tiles = tok_rows // TILE
    blocks_here = prefix_keys.shape[0] // BLOCK
    peers = lax.axis_size("ctx")
    me, core = lax.axis_index("ctx"), lax.axis_index("head")
    requests = tiles * heads * TOPK
    capacity = -(-requests // (peers * blocks_here))
    slots = capacity * blocks_here
    swap = [(0, 1), (1, 0)]
    both = ("ctx", "head")

    orders = bit_orders(peers)
    steps = len(orders[0])

    def gathered(weight):
        for step in range(steps - 3):
            got = lax.ppermute(weight, both, doubling_pairs(peers, orders, step))
            weight = joined(weight, got)
        pieces = [weight]
        for step in range(steps - 3, steps - 1):
            pairs = doubling_pairs(peers, orders, step)
            pieces += [lax.ppermute(piece, both, pairs) for piece in pieces]
        mine, theirs = stacked_halves(pieces, core)
        far_own = lax.ppermute(mine, both, doubling_pairs(peers, orders, steps - 1))
        far_other = lax.ppermute(theirs, both, doubling_pairs(peers, orders, steps - 1, True))
        near_other = lax.ppermute(theirs, "head", swap)
        return mine, far_own, near_other, far_other

    weights = [gathered(out_weight[0])]

    parts = [slots]
    outgoing, owner, rank = route_queries(
        selected.reshape(requests), queries, peers, parts, blocks_here
    )
    incoming = []
    for sent in outgoing:
        incoming.append(lax.all_to_all(sent, "ctx", split_axis=0, concat_axis=0, tiled=True))
    own_out, own_lse, turned = own_attention(queries, keys, values, prefix_values)

    apart = jnp.arange(peers, dtype=jnp.int32) ^ me
    places = [sum(((apart >> bit) & 1) << k for k, bit in enumerate(order)) for order in orders]
    place = jnp.where(core == 0, places[0], places[1])

    backs = []
    for n, asked in zip(parts, incoming):
        pairs = asked[:, n * TILE : n * TILE + n, 0].astype(jnp.int32).reshape(peers * n)
        answers = attend_slots(pairs, asked, prefix_keys, turned, n, heads)
        backs.append(lax.all_to_all(answers, "ctx", split_axis=0, concat_axis=0, tiled=True))
    att = combine(owner, rank, place, backs, own_out, own_lse, parts)
    att_other = lax.ppermute(att, "head", swap)
    return project(att, att_other, weights)


def solution(mesh):
    return jax.shard_map(
        shards,
        mesh=mesh,
        in_specs=(
            P("ctx", "head"),
            P("ctx", "head"),
            P("ctx", "head"),
            P("ctx", "head"),
            P("ctx", "head"),
            P("head", "ctx", None, None),
            P("head", "ctx", None),
        ),
        out_specs=P("ctx", "head"),
        check_vma=False,
    )
```
